32 devices in a mesh: dp: 4 (over y, z), fsdp: 8 (over x, core).
Axes of the slice: x: 4, y: 2, z: 2, core: 2. Of those that a mesh axis runs over, the one named last changes fastest.
The devices are a block of a 4x4x8 slice.
Arguments:
- x: bfloat16 [128, 512, 1152], P(('dp', 'fsdp')), parts along dimension 0
- w_q: bfloat16 [2, 1152, 1024], P(None, 'fsdp')
- w_k: bfloat16 [2, 1152, 256], P(None, 'fsdp')
- w_v: bfloat16 [2, 1152, 256], P(None, 'fsdp')
- w_o: bfloat16 [2, 1024, 1152], P(None, 'fsdp')
- w_gate: bfloat16 [2, 1152, 6912], P(None, 'fsdp')
- w_up: bfloat16 [2, 1152, 6912], P(None, 'fsdp')
- w_down: bfloat16 [2, 6912, 1152], P(None, 'fsdp')
- norm_w: float32 [2, 4, 1152], replicated
- qk_norm_w: float32 [2, 2, 256], replicated
Outputs:
- output 1: bfloat16 [128, 512, 1152], P(('dp', 'fsdp')), parts along dimension 0
- output 2: bfloat16 [128, 512, 1, 256], P(('dp', 'fsdp')), parts along dimension 0
- output 3: bfloat16 [128, 512, 1, 256], P(('dp', 'fsdp')), parts along dimension 0
There are 4 independent parts. The reference program is written for one: setup_inputs(seed, part) draws one part's arguments, and reference() takes and returns one part's arrays. A program takes and returns all parts, laid end to end along the dimension named above; an argument that names none is the same for every part.
All inputs are finite; a program needn't handle non-finite values.
Results may differ from the reference program's by a relative error of at most 0.0169795.
Values are sent between devices in bfloat16 or wider.
A program may use at most 768 MiB of HBM per device.

```python
import jax
import jax.numpy as jnp
from jax import lax

MODEL_DIM = 1152
NUM_HEADS = 4
KV_HEADS = 1
HEAD_DIM = 256
FFN_DIM = 6912
WINDOW = 1024
NUM_SEQS = 32
SEQ_LEN = 512

NORM_EPS = 1e-6
LOCAL_BASE = 10000.0
GLOBAL_BASE = 1000000.0
GLOBAL_POS_DIV = 8.0


def setup_inputs(seed: int = 0, part: int = 0) -> dict:
    base_key = jax.random.key(seed)
    sub_keys = jax.random.split(base_key, 10)
    x_key = jax.random.fold_in(sub_keys[0], part)
    q_width = NUM_HEADS * HEAD_DIM
    kv_width = KV_HEADS * HEAD_DIM

    def draw_weight(rand_key, fan_in, fan_out):
        values = jax.random.normal(rand_key, (2, fan_in, fan_out), jnp.float32) * fan_in ** -0.5
        return values.astype(jnp.bfloat16)

    return {
        'x': jax.random.normal(x_key, (NUM_SEQS, SEQ_LEN, MODEL_DIM), jnp.float32).astype(jnp.bfloat16),
        'w_q': draw_weight(sub_keys[1], MODEL_DIM, q_width),
        'w_k': draw_weight(sub_keys[2], MODEL_DIM, kv_width),
        'w_v': draw_weight(sub_keys[3], MODEL_DIM, kv_width),
        'w_o': draw_weight(sub_keys[4], q_width, MODEL_DIM),
        'w_gate': draw_weight(sub_keys[5], MODEL_DIM, FFN_DIM),
        'w_up': draw_weight(sub_keys[6], MODEL_DIM, FFN_DIM),
        'w_down': draw_weight(sub_keys[7], FFN_DIM, MODEL_DIM),
        'norm_w': 0.3 * jax.random.normal(sub_keys[8], (2, 4, MODEL_DIM), jnp.float32),
        'qk_norm_w': 0.3 * jax.random.normal(sub_keys[9], (2, 2, HEAD_DIM), jnp.float32),
    }


def rms_norm(values, gain_w):
    mean_sq = jnp.mean(values * values, axis=-1, keepdims=True)
    return values * lax.rsqrt(mean_sq + NORM_EPS) * (1.0 + gain_w)


def rope_tables(rope_base, pos_div):
    half_dim = HEAD_DIM // 2
    inv_freq = rope_base ** (-2.0 * jnp.arange(half_dim, dtype=jnp.float32) / HEAD_DIM)
    positions = jnp.arange(SEQ_LEN, dtype=jnp.float32) / pos_div
    angles = positions[:, None] * inv_freq[None, :]
    return jnp.cos(angles), jnp.sin(angles)


def apply_rope(values, cos_t, sin_t):
    half_dim = values.shape[-1] // 2
    lo_half = values[..., :half_dim]
    hi_half = values[..., half_dim:]
    cos_b = cos_t[:, None, :]
    sin_b = sin_t[:, None, :]
    return jnp.concatenate([lo_half * cos_b - hi_half * sin_b, hi_half * cos_b + lo_half * sin_b], axis=-1)


def attend(query_bf, key_bf, value_bf, window):
    groups = NUM_HEADS // KV_HEADS
    q_scalar = MODEL_DIM // NUM_HEADS if HEAD_DIM == 128 else HEAD_DIM
    q_scale = q_scalar ** -0.5
    q_block = min(SEQ_LEN, 512)
    num_blocks = SEQ_LEN // q_block
    query_grp = query_bf.astype(jnp.float32).reshape(num_blocks, q_block, KV_HEADS, groups, HEAD_DIM)
    key_f32 = key_bf.astype(jnp.float32)
    value_f32 = value_bf.astype(jnp.float32)
    key_pos = jnp.arange(SEQ_LEN)

    def one_block(block_args):
        blk_idx, q_blk = block_args
        q_pos = blk_idx * q_block + jnp.arange(q_block)
        scores = jnp.einsum('qkgd,skd->kgqs', q_blk, key_f32) * q_scale
        pos_diff = q_pos[:, None] - key_pos[None, :]
        allowed = (pos_diff >= 0) & (pos_diff < window)
        scores = jnp.where(allowed, scores, -1e30)
        probs_bf = jax.nn.softmax(scores, axis=-1).astype(jnp.bfloat16)
        block_out = jnp.einsum('kgqs,skd->qkgd', probs_bf.astype(jnp.float32), value_f32)
        return block_out.astype(jnp.bfloat16)

    block_outs = lax.map(one_block, (jnp.arange(num_blocks), query_grp))
    return block_outs.reshape(SEQ_LEN, NUM_HEADS * HEAD_DIM)


def decoder_layer(x_seq, weights, norm_w, qk_norm_w, window, rope_base, pos_div):
    w_q, w_k, w_v, w_o, w_gate, w_up, w_down = weights
    x_f32 = x_seq.astype(jnp.float32)
    normed = rms_norm(x_f32, norm_w[0]).astype(jnp.bfloat16)
    query_f32 = jnp.dot(normed, w_q, preferred_element_type=jnp.float32).reshape(SEQ_LEN, NUM_HEADS, HEAD_DIM)
    key_f32 = jnp.dot(normed, w_k, preferred_element_type=jnp.float32).reshape(SEQ_LEN, KV_HEADS, HEAD_DIM)
    value_bf = jnp.dot(normed, w_v, preferred_element_type=jnp.float32).astype(jnp.bfloat16).reshape(SEQ_LEN, KV_HEADS, HEAD_DIM)
    cos_t, sin_t = rope_tables(rope_base, pos_div)
    query_bf = apply_rope(rms_norm(query_f32, qk_norm_w[0]), cos_t, sin_t).astype(jnp.bfloat16)
    key_bf = apply_rope(rms_norm(key_f32, qk_norm_w[1]), cos_t, sin_t).astype(jnp.bfloat16)
    attn_out = attend(query_bf, key_bf, value_bf, window)
    attn_proj = jnp.dot(attn_out, w_o, preferred_element_type=jnp.float32)
    resid = (x_f32 + rms_norm(attn_proj, norm_w[1])).astype(jnp.bfloat16)
    resid_f32 = resid.astype(jnp.float32)
    normed_ffn = rms_norm(resid_f32, norm_w[2]).astype(jnp.bfloat16)
    gate_f32 = jnp.dot(normed_ffn, w_gate, preferred_element_type=jnp.float32)
    up_f32 = jnp.dot(normed_ffn, w_up, preferred_element_type=jnp.float32)
    hidden_act = (jax.nn.gelu(gate_f32, approximate=True) * up_f32).astype(jnp.bfloat16)
    down_f32 = jnp.dot(hidden_act, w_down, preferred_element_type=jnp.float32)
    layer_out = (resid_f32 + rms_norm(down_f32, norm_w[3])).astype(jnp.bfloat16)
    return layer_out, key_bf, value_bf


def reference(x, w_q, w_k, w_v, w_o, w_gate, w_up, w_down, norm_w, qk_norm_w):
    stacked = (w_q, w_k, w_v, w_o, w_gate, w_up, w_down)
    local_w = tuple(w_all[0] for w_all in stacked)
    global_w = tuple(w_all[1] for w_all in stacked)

    def one_seq(x_seq):
        hidden = decoder_layer(x_seq, local_w, norm_w[0], qk_norm_w[0], WINDOW, LOCAL_BASE, 1.0)[0]
        return decoder_layer(hidden, global_w, norm_w[1], qk_norm_w[1], SEQ_LEN, GLOBAL_BASE, GLOBAL_POS_DIV)

    x_out, k_cache, v_cache = lax.map(one_seq, x)
    return (x_out, k_cache, v_cache)
```

```python
import functools
import math

import jax
import jax.numpy as jnp
from jax import lax
from jax.experimental import pallas as pl
from jax.experimental.pallas import tpu as pltpu
from jax.sharding import PartitionSpec as P

WINDOW = 1024
NORM_EPS = 1e-6
LOCAL_BASE = 10000.0
GLOBAL_BASE = 1000000.0
GLOBAL_POS_DIV = 8.0
MESH = pl.DeviceIdType.MESH
F32 = jnp.float32
BF16 = jnp.bfloat16
LAYERS = 2
CHUNKS = 9
SPLIT = 2
ROW_BLOCKS = 4
DUNITS = 9
GELU_A = math.sqrt(2.0 / math.pi)
GELU_B = GELU_A * 0.044715

T_ATT, T_GU, T_DN = 47, 21, 93
PACE = 38
START = dict(A=3, B=1, C=1, N=1, D=1)
LAG = dict(A=3 * PACE, B=2 * PACE - 20, C=PACE, N=-70, D=-90)


def rope_tables(seq_len, head_dim, rope_base, pos_div):
    half_dim = head_dim // 2
    inv_freq = rope_base ** (-2.0 * jnp.arange(half_dim, dtype=F32) / head_dim)
    positions = jnp.arange(seq_len, dtype=F32) / pos_div
    angles = positions[:, None] * inv_freq[None, :]
    return jnp.cos(angles), jnp.sin(angles)


def rms(values, gain_w):
    mean_sq = jnp.mean(values * values, axis=-1, keepdims=True)
    return values * lax.rsqrt(mean_sq + NORM_EPS) * (1.0 + gain_w)


def dot(a, b):
    return jnp.dot(a, b, preferred_element_type=F32)


def kernel(cfg, x_in, wq, wk, wv, wo, wg, wu, wd, nw, qkn, cos, sin,
           x_out, k_out, v_out, fq, fk, fv, fo, fg, fu, fd,
           xbuf, gbuf, ubuf, fbuf, wgb, wub, wdb,
           loc, s_own, s_rel, s_par, s_sib, r_left, r_right, r_opp, r_par, r_sib,
           ld_x, ld_att, ld_gu, ld_dn, st_kv, st_x):
    ring, nz, use_z, use_y = cfg
    nseq, seq, dim = xbuf.shape
    rows_in, rows_o, rows_d = wq.shape[1], wo.shape[1], wd.shape[1]
    qw, kw, ffn = wq.shape[2], wk.shape[2], wg.shape[2]
    head = qkn.shape[-1]
    heads = qw // head
    chunk = ffn // CHUNKS
    gu_units = CHUNKS * SPLIT
    guw = ffn // gu_units
    drows = rows_d // DUNITS
    per_layer = 2 + gu_units + DUNITS
    total = LAYERS * per_layer

    dp = lax.axis_index("dp")
    me = lax.axis_index("fsdp")
    pos, core = me // 2, me % 2
    left_pos, right_pos = (pos + ring - 1) % ring, (pos + 1) % ring
    opp_pos = (pos + 2) % ring
    right = (dp, right_pos * 2 + core)
    left = (dp, left_pos * 2 + core)
    sibling = (dp, pos * 2 + 1 - core)
    zb = dp % 2
    yb = (dp // nz) % 2
    color = ((zb if use_z else 0) + (yb if use_y else 0)) % 2
    z_peer = (dp + 1 - 2 * zb, me)
    y_peer = (dp + nz * (1 - 2 * yb), me)
    peers = [right, left, sibling]
    if use_z:
        peers.append(z_peer)
    if use_y:
        peers.append(y_peer)

    barrier = pltpu.get_barrier_semaphore()
    for peer in peers:
        pl.semaphore_signal(barrier, inc=1, device_id=peer, device_id_type=MESH)
    pl.semaphore_wait(barrier, len(peers))

    class Unit:
        pass

    def unit(kind, l, j):
        u = Unit()
        u.kind, u.shared = kind, False
        if kind == "qkv":
            u.parts = [(wq, fq), (wk, fk), (wv, fv)]
            u.own = lambda w: w.at[l]
            u.full = lambda f, x, c: f.at[l, x, c]
            u.half = rows_in // 2
            u.cut = lambda f, x, c, h: f.at[l, x, c, pl.ds(h * u.half, u.half)]
            u.bytes = lambda n: fg.at[0, pl.ds(0, n), 0, :, pl.ds(0, qw + 2 * kw)]
        elif kind == "o":
            u.parts = [(wo, fo)]
            u.own = lambda w: w.at[l]
            u.full = lambda f, x, c: f.at[l, x, c]
            u.half = rows_o // 2
            u.cut = lambda f, x, c, h: f.at[l, x, c, pl.ds(h * u.half, u.half)]
            u.bytes = lambda n: fo.at[0, pl.ds(0, n), 0]
        elif kind == "gu":
            col = pl.multiple_of(j * guw, guw)
            u.parts = [(wg, fg), (wu, fu)]
            u.own = lambda w: w.at[l, :, pl.ds(col, guw)]
            u.full = lambda f, x, c: f.at[l, x, c, :, pl.ds(col, guw)]
            u.half = rows_in // 2
            u.cut = lambda f, x, c, h: f.at[l, x, c, pl.ds(h * u.half, u.half), pl.ds(col, guw)]
            u.bytes = lambda n: fg.at[0, pl.ds(0, n), 0, :, pl.ds(0, 2 * guw)]
            u.shared = True
        else:
            row = pl.multiple_of(j * drows, drows)
            u.parts = [(wd, fd)]
            u.own = lambda w: w.at[l, pl.ds(row, drows)]
            u.full = lambda f, x, c: f.at[l, x, c, pl.ds(row, drows)]
            u.half = drows // 2
            u.cut = lambda f, x, c, h: f.at[l, x, c, pl.ds(pl.multiple_of(row + h * u.half, u.half), u.half)]
            u.bytes = lambda n: fd.at[0, pl.ds(0, n), 0, pl.ds(0, drows)]
            u.shared = True
        u.pair = not u.shared or not (use_z or use_y)
        u.fetch = None if u.pair else (color == j % 2)
        u.over_y = (j // 2) % 2
        return u

    def per_class(p, fn):
        l = p // per_layer
        q = p % per_layer

        @pl.when(q == 0)
        def _():
            fn(unit("qkv", l, 0), p)

        @pl.when(q == 1)
        def _():
            fn(unit("o", l, 0), p)

        @pl.when((q >= 2) & (q < 2 + gu_units))
        def _():
            fn(unit("gu", l, q - 2), p)

        @pl.when(q >= 2 + gu_units)
        def _():
            fn(unit("d", l, q - 2 - gu_units), p)

    def fetching(u, fn):
        if u.fetch is None:
            fn()
        else:
            pl.when(u.fetch)(fn)

    def on_peer(u, fn):
        if u.pair:
            return
        if use_z and use_y:
            pl.when(u.over_y == 0)(lambda: fn(z_peer))
            pl.when(u.over_y == 1)(lambda: fn(y_peer))
        else:
            fn(z_peer if use_z else y_peer)

    def wait(sem, ref):
        pltpu.make_async_copy(ref, ref, sem).wait()

    def send(src, dst, s_sem, r_sem, device):
        pltpu.make_async_remote_copy(src, dst, s_sem, r_sem, device_id=device, device_id_type=MESH).start()

    def stage_a(u, p):
        for w, f in u.parts:
            pltpu.make_async_copy(u.own(w), u.full(f, pos, core), loc.at[p]).start()

        def go():
            for w, f in u.parts:
                send(u.own(w), u.full(f, pos, core), s_own.at[p], r_left.at[p], right)
                send(u.own(w), u.full(f, pos, core), s_own.at[p], r_right.at[p], left)

        fetching(u, go)

    def stage_b(u, p):
        def go():
            wait(r_left.at[p], u.bytes(1))
            wait(r_right.at[p], u.bytes(1))
            for _, f in u.parts:
                send(u.cut(f, left_pos, core, 0), u.cut(f, left_pos, core, 0), s_rel.at[p], r_opp.at[p], right)
                send(u.cut(f, right_pos, core, 1), u.cut(f, right_pos, core, 1), s_rel.at[p], r_opp.at[p], left)

            def share(peer):
                for _, f in u.parts:
                    for x in (left_pos, right_pos):
                        send(u.full(f, x, core), u.full(f, x, core), s_par.at[p], r_par.at[p], peer)

            on_peer(u, share)

        fetching(u, go)

    def stage_c(u, p):
        def go():
            wait(r_opp.at[p], u.bytes(1))

            def share(peer):
                for _, f in u.parts:
                    send(u.full(f, opp_pos, core), u.full(f, opp_pos, core), s_par.at[p], r_par.at[p], peer)

            on_peer(u, share)

        fetching(u, go)

    def stage_n(u, p):
        if not u.pair:
            pl.when(jnp.logical_not(u.fetch))(lambda: wait(r_par.at[p], u.bytes(ring - 1)))

    def stage_d(u, p):
        wait(loc.at[p], u.bytes(1))
        for _, f in u.parts:
            src = u.full(f, pl.ds(0, ring), core)
            send(src, src, s_sib.at[p], r_sib.at[p], sibling)

    def stage_e(u, p):
        wait(r_sib.at[p], u.bytes(ring))

    def drain(u, p):
        def go():
            wait(s_own.at[p], u.bytes(2))
            wait(s_rel.at[p], u.bytes(1))
            if not u.pair:
                wait(s_par.at[p], u.bytes(ring - 1))

        fetching(u, go)
        wait(s_sib.at[p], u.bytes(ring))

    def count(v, s):
        return jnp.clip((v + LAG[s]) // PACE, 0, total)

    order = [("A", stage_a), ("B", stage_b), ("C", stage_c), ("N", stage_n), ("D", stage_d)]

    att_steps, gu_steps, dn_steps = 2 * nseq, CHUNKS * nseq, nseq
    t_layer = att_steps * T_ATT + gu_steps * T_GU + dn_steps * T_DN
    steps = att_steps + gu_steps + dn_steps

    def when_of(k):
        l, i = k // steps, k % steps
        att = jnp.minimum(i, att_steps)
        gu = jnp.clip(i - att_steps, 0, gu_steps)
        dn = jnp.maximum(i - att_steps - gu_steps, 0)
        return l * t_layer + att * T_ATT + gu * T_GU + dn * T_DN

    def reached(k, s):
        l, i = k // steps, k % steps
        chunks = jnp.clip((i + nseq - att_steps) // nseq + 1, 0, CHUNKS)
        need = jnp.where(i >= nseq, 2, 1)
        need = jnp.where(i >= att_steps - 1, 2 + SPLIT * chunks, need)
        need = jnp.where(i >= att_steps + gu_steps, per_layer, need)
        return jnp.maximum(jnp.maximum(count(when_of(k), s), l * per_layer + need), START[s])

    def tick(k):
        for s, fn in order:
            lo = jnp.where(k == 0, START[s], reached(jnp.maximum(k - 1, 0), s))
            lax.fori_loop(lo, reached(k, s), lambda p, c, fn=fn: (per_class(p, fn), c)[1], 0)

    pltpu.make_async_copy(x_in, xbuf, ld_x).start()
    first = unit("qkv", 0, 0)
    stage_a(first, 0)
    stage_b(first, 0)
    for p in range(1, START["A"]):
        q = [unit("o", 0, 0), unit("gu", 0, 0)][p - 1]
        stage_a(q, p)
    stage_c(first, 0)
    stage_n(first, 0)
    stage_d(first, 0)
    wait(ld_x, xbuf)

    att_o = ubuf.at[pl.ds(0, seq), pl.ds(qw + 2 * kw, qw)]
    att_h = ubuf.at[pl.ds(0, seq), pl.ds(2 * (qw + kw), dim)]

    def by_rows(fn):
        block = seq // ROW_BLOCKS
        lax.fori_loop(0, ROW_BLOCKS, lambda r, c: (fn(pl.ds(pl.multiple_of(r * block, block), block)), c)[1], 0)

    def kv_rows(s):
        return pl.ds(pl.multiple_of(s * seq, seq), seq)

    def load_gu(l, j):
        slot = j % 2
        col = pl.multiple_of(j * chunk, chunk)
        for f, b, n in ((fg, wgb, 0), (fu, wub, 1)):
            pltpu.make_async_copy(f.at[l, :, :, :, pl.ds(col, chunk)], b.at[slot], ld_gu.at[slot, n]).start()

    def arrive_gu(l, j):
        for n in range(SPLIT):
            stage_e(unit("gu", l, j * SPLIT + n), l * per_layer + 2 + j * SPLIT + n)

    def attention_in(l, s):
        @pl.when(s == 0)
        def _():
            stage_e(unit("qkv", l, 0), l * per_layer)
            copies = [
                (fq.at[l], wdb.at[:, :, pl.ds(0, rows_in), pl.ds(0, qw)]),
                (fk.at[l], wdb.at[:, :, pl.ds(rows_in, rows_in), pl.ds(0, kw)]),
                (fv.at[l], wdb.at[:, :, pl.ds(rows_in, rows_in), pl.ds(kw, kw)]),
            ]
            copies = [pltpu.make_async_copy(a, b, ld_att.at[n]) for n, (a, b) in enumerate(copies)]
            for c in copies:
                c.start()
            for c in copies:
                c.wait()


        def norm(rows):
            att_h[rows, :] = rms(xbuf[s, rows, :].astype(F32), nw[l, 0:1]).astype(BF16)

        by_rows(norm)
        cos_t, sin_t = cos[l], sin[l]

        def turn(v, gain):
            v = rms(v, gain)
            lo, hi = v[:, : head // 2], v[:, head // 2 :]
            return jnp.concatenate([lo * cos_t - hi * sin_t, hi * cos_t + lo * sin_t], axis=-1).astype(BF16)

        def project(row, col):
            return dot(att_h[...], wdb[:, :, row : row + rows_in, col : col + kw].reshape(dim, kw))

        ubuf[kv_rows(s), qw : qw + kw] = turn(project(rows_in, 0), qkn[l, 1:2])
        ubuf[kv_rows(s), qw + kw : qw + 2 * kw] = project(rows_in, kw).astype(BF16)
        for n in range(heads):
            ubuf[kv_rows(s), n * head : (n + 1) * head] = turn(project(0, n * head), qkn[l, 0:1])

        @pl.when(l == LAYERS - 1)
        def _():
            for f, at, n in ((k_out, qw, 0), (v_out, qw + kw, 1)):
                pltpu.make_async_copy(ubuf.at[kv_rows(s), pl.ds(at, kw)], f.at[s], st_kv.at[n, s]).start()

    def attention_out(l, s):
        @pl.when(s == 0)
        def _():
            stage_e(unit("o", l, 0), l * per_layer + 1)
            c = pltpu.make_async_copy(fo.at[l], wdb.at[:, :, pl.ds(2 * rows_in, rows_o), :], ld_att.at[3])
            c.start()
            c.wait()

        @pl.when(s == nseq - 1)
        def _():
            arrive_gu(l, 0)
            load_gu(l, 0)

        scale = head**-0.5
        blk = seq // 2
        for n in range(heads):
            for b in range(2):
                span = (b + 1) * blk
                q = ubuf[pl.ds(pl.multiple_of(s * seq + b * blk, blk), blk), n * head : (n + 1) * head]
                k = ubuf[pl.ds(pl.multiple_of(s * seq, seq), span), qw : qw + kw]
                v = ubuf[pl.ds(pl.multiple_of(s * seq, seq), span), qw + kw : qw + 2 * kw]
                sc = lax.dot_general(q, k, (((1,), (1,)), ((), ())), preferred_element_type=F32) * scale
                qpos = lax.broadcasted_iota(jnp.int32, (blk, span), 0) + b * blk
                kpos = lax.broadcasted_iota(jnp.int32, (blk, span), 1)
                sc = jnp.where(qpos >= kpos, sc, -1e30)
                e = jnp.exp(sc - jnp.max(sc, axis=-1, keepdims=True))
                pr = (e / jnp.sum(e, axis=-1, keepdims=True)).astype(BF16)
                att_o[b * blk : (b + 1) * blk, n * head : (n + 1) * head] = dot(pr, v).astype(BF16)
        for n in range(0, dim, 256):
            cols = slice(n, min(n + 256, dim))
            fbuf[:, cols] = dot(att_o[...], wdb[:, :, 2 * rows_in : 2 * rows_in + rows_o, cols].reshape(qw, -1))

        def close(rows):
            x1 = (xbuf[s, rows, :].astype(F32) + rms(fbuf[rows, :], nw[l, 1:2])).astype(BF16)
            xbuf[s, rows, :] = x1
            gbuf[s, rows, :] = rms(x1.astype(F32), nw[l, 2:3]).astype(BF16)

        by_rows(close)

        @pl.when((s == nseq - 1) & (l == LAYERS - 1))
        def _():
            for f, at, n in ((k_out, qw, 0), (v_out, qw + kw, 1)):
                for t in range(nseq):
                    pltpu.make_async_copy(ubuf.at[kv_rows(t), pl.ds(at, kw)], f.at[t], st_kv.at[n, t]).wait()

    def gate_up(l, j, m):
        slot = j % 2

        @pl.when(m == 0)
        def _():
            for b, n in ((wgb, 0), (wub, 1)):
                wait(ld_gu.at[slot, n], b.at[slot])

            @pl.when(j + 1 < CHUNKS)
            def _():
                arrive_gu(l, j + 1)
                load_gu(l, j + 1)


        step = min(256, chunk)
        for n in range(0, chunk, step):
            gate = dot(gbuf[m], wgb[slot, :, :, :, n : n + step].reshape(dim, step))
            up = dot(gbuf[m], wub[slot, :, :, :, n : n + step].reshape(dim, step))
            half = 0.5 * gate
            t = jnp.tanh(gate * (GELU_A + GELU_B * (gate * gate)))
            cols = pl.ds(pl.multiple_of(j * chunk + n, step), step)
            ubuf[kv_rows(m), cols] = ((half + half * t) * up).astype(BF16)

    def down(l, m):
        @pl.when(m == 0)
        def _():
            for n in range(DUNITS):
                stage_e(unit("d", l, n), l * per_layer + 2 + gu_units + n)
                at = pl.ds(n * drows, drows)
                pltpu.make_async_copy(fd.at[l, :, :, at], wdb.at[:, :, at], ld_dn).start()
            wait(ld_dn, wdb)

        for n in range(0, dim, 256):
            cols = slice(n, min(n + 256, dim))
            fbuf[:, cols] = dot(ubuf[kv_rows(m), :], wdb[:, :, :, cols].reshape(ffn, -1))

        def close(rows):
            xbuf[m, rows, :] = (xbuf[m, rows, :].astype(F32) + rms(fbuf[rows, :], nw[l, 3:4])).astype(BF16)

        by_rows(close)

        @pl.when(l == LAYERS - 1)
        def _():
            pltpu.make_async_copy(xbuf.at[m], x_out.at[m], st_x.at[m]).start()

    def body(k, carry):
        tick(k)
        l, i = k // steps, k % steps

        @pl.when(i < nseq)
        def _():
            attention_in(l, i)

        @pl.when((i >= nseq) & (i < att_steps))
        def _():
            attention_out(l, i - nseq)

        @pl.when((i >= att_steps) & (i < att_steps + gu_steps))
        def _():
            gate_up(l, (i - att_steps) // nseq, (i - att_steps) % nseq)

        @pl.when(i >= att_steps + gu_steps)
        def _():
            down(l, i - att_steps - gu_steps)

        return carry

    lax.fori_loop(0, LAYERS * steps, body, 0)

    for m in range(nseq):
        pltpu.make_async_copy(xbuf.at[m], x_out.at[m], st_x.at[m]).wait()
    lax.fori_loop(0, total, lambda p, c: (per_class(p, drain), c)[1], 0)


def layout(mesh):
    n = mesh.shape["dp"]
    lead = [getattr(d, "coords", None) for d in mesh.devices.reshape(n, -1)[:, 0]]
    nz = n
    if all(c is not None for c in lead):
        nz = next((i for i in range(1, n) if lead[i][1] != lead[0][1]), n)
    return nz, nz % 2 == 0, n % nz == 0 and (n // nz) % 2 == 0


def solution(mesh):
    batch_spec = P(("dp", "fsdp"), None, None)
    cache_spec = P(("dp", "fsdp"), None, None, None)
    weight_spec = P(None, "fsdp", None)
    rep_spec = P()
    ring = mesh.shape["fsdp"] // 2
    cfg = (ring,) + layout(mesh)

    def per_device(x, w_q, w_k, w_v, w_o, w_gate, w_up, w_down, norm_w, qk_norm_w):
        weights = (w_q, w_k, w_v, w_o, w_gate, w_up, w_down)
        nseq, seq, dim = x.shape
        head = qk_norm_w.shape[-1]
        ffn = w_gate.shape[2]
        kw = w_k.shape[2]
        assert seq <= WINDOW and kw == head and ring == 4
        tables = [rope_tables(seq, head, LOCAL_BASE, 1.0), rope_tables(seq, head, GLOBAL_BASE, GLOBAL_POS_DIV)]
        cos = jnp.stack([t[0] for t in tables])
        sin = jnp.stack([t[1] for t in tables])
        units = LAYERS * (2 + CHUNKS * SPLIT + DUNITS)
        hbm = pl.BlockSpec(memory_space=pl.ANY)
        vmem = pl.BlockSpec(memory_space=pltpu.VMEM)
        outs = [
            jax.ShapeDtypeStruct(x.shape, BF16),
            jax.ShapeDtypeStruct((nseq, seq, kw), BF16),
            jax.ShapeDtypeStruct((nseq, seq, kw), BF16),
        ] + [jax.ShapeDtypeStruct((LAYERS, ring, 2) + w.shape[1:], BF16) for w in weights]
        rows_d = w_down.shape[1]
        res = pl.pallas_call(
            functools.partial(kernel, cfg),
            out_shape=outs,
            in_specs=[hbm] * 8 + [vmem] * 4,
            out_specs=[hbm] * len(outs),
            scratch_shapes=[
                pltpu.VMEM((nseq, seq, dim), BF16),
                pltpu.VMEM((nseq, seq, dim), BF16),
                pltpu.VMEM((nseq * seq, ffn), BF16),
                pltpu.VMEM((seq, dim), F32),
                pltpu.VMEM((2, ring, 2, w_gate.shape[1], ffn // CHUNKS), BF16),
                pltpu.VMEM((2, ring, 2, w_gate.shape[1], ffn // CHUNKS), BF16),
                pltpu.VMEM((ring, 2, rows_d, dim), BF16),
            ]
            + [pltpu.SemaphoreType.DMA((units,)) for _ in range(10)]
            + [
                pltpu.SemaphoreType.DMA,
                pltpu.SemaphoreType.DMA((4,)),
                pltpu.SemaphoreType.DMA((2, 2)),
                pltpu.SemaphoreType.DMA,
                pltpu.SemaphoreType.DMA((2, nseq)),
                pltpu.SemaphoreType.DMA((nseq,)),
            ],
            compiler_params=pltpu.CompilerParams(
                collective_id=0, has_side_effects=True, vmem_limit_bytes=67_043_328
            ),
        )(x, *weights, norm_w, qk_norm_w, cos, sin)
        shape = (nseq, seq, 1, kw)
        return res[0], res[1].reshape(shape), res[2].reshape(shape)

    in_specs = (batch_spec,) + (weight_spec,) * 7 + (rep_spec, rep_spec)
    return jax.shard_map(per_device, mesh=mesh, in_specs=in_specs, out_specs=(batch_spec, cache_spec, cache_spec), check_vma=False)
```

```python
import functools
import math

import jax
import jax.numpy as jnp
from jax import lax
from jax.experimental import pallas as pl
from jax.experimental.pallas import tpu as pltpu
from jax.sharding import PartitionSpec as P

WINDOW = 1024
NORM_EPS = 1e-6
LOCAL_BASE = 10000.0
GLOBAL_BASE = 1000000.0
GLOBAL_POS_DIV = 8.0
MESH = pl.DeviceIdType.MESH
F32 = jnp.float32
BF16 = jnp.bfloat16
LAYERS = 2
CHUNKS = 9
SPLIT = 2
EARLY = 1
LATE_D = 2
ROW_BLOCKS = 4
DUNITS = 6
GELU_A = math.sqrt(2.0 / math.pi)
GELU_B = GELU_A * 0.044715

T_ATT, T_GU, T_DN = 34, 21, 93
PACE = (36, 45)
LAG = (dict(A=249, B=169, C=63, N=-51, D=-59), dict(A=690, B=549, C=415, N=188, D=188))
START = dict(A=4, B=1, C=1, N=1, D=1)


def rope_tables(seq_len, head_dim):
    half_dim = head_dim // 2
    exponent = -2.0 * jnp.arange(half_dim, dtype=F32) / head_dim
    inv_freq = jnp.stack([LOCAL_BASE**exponent, GLOBAL_BASE**exponent])
    positions = jnp.arange(seq_len, dtype=F32)
    positions = jnp.stack([positions, positions / GLOBAL_POS_DIV])
    angles = positions[:, :, None] * inv_freq[:, None, :]
    return jnp.cos(angles), jnp.sin(angles)


def rms(values, gain_w):
    mean_sq = jnp.mean(values * values, axis=-1, keepdims=True)
    return values * lax.rsqrt(mean_sq + NORM_EPS) * (1.0 + gain_w)


def dot(a, b):
    return jnp.dot(a, b, preferred_element_type=F32)


def kernel(cfg, x_in, wq, wk, wv, wo, wg, wu, wd, nw, qkn, cos, sin,
           x_out, k_out, v_out, fq, fk, fv, fo, fg, fu, fd,
           xbuf, gbuf, ubuf, fbuf, wgb, wub, wdb,
           loc, s_own, s_rel, s_par, s_sib, r_left, r_right, r_opp, r_par, r_sib,
           ld_x, ld_att, ld_gu, ld_dn, st_kv, st_x):
    ring, nz, use_z, use_y = cfg
    nseq, seq, dim = xbuf.shape
    rows_in, rows_o, rows_d = wq.shape[1], wo.shape[1], wd.shape[1]
    qw, kw, ffn = wq.shape[2], wk.shape[2], wg.shape[2]
    head = qkn.shape[-1]
    heads = qw // head
    chunk = ffn // CHUNKS
    gu_units = CHUNKS * SPLIT
    guw = ffn // gu_units
    drows = rows_d // DUNITS
    per_layer = 2 + gu_units + DUNITS
    total = LAYERS * per_layer

    dp = lax.axis_index("dp")
    me = lax.axis_index("fsdp")
    pos, core = me // 2, me % 2
    left_pos, right_pos = (pos + ring - 1) % ring, (pos + 1) % ring
    opp_pos = (pos + 2) % ring
    right = (dp, right_pos * 2 + core)
    left = (dp, left_pos * 2 + core)
    sibling = (dp, pos * 2 + 1 - core)
    zb = dp % 2
    yb = (dp // nz) % 2
    color = ((zb if use_z else 0) + (yb if use_y else 0)) % 2
    z_peer = (dp + 1 - 2 * zb, me)
    y_peer = (dp + nz * (1 - 2 * yb), me)
    peers = [right, left, sibling]
    if use_z:
        peers.append(z_peer)
    if use_y:
        peers.append(y_peer)

    barrier = pltpu.get_barrier_semaphore()
    for peer in peers:
        pl.semaphore_signal(barrier, inc=1, device_id=peer, device_id_type=MESH)
    pl.semaphore_wait(barrier, len(peers))

    class Unit:
        pass

    def unit(kind, l, j):
        u = Unit()
        u.kind, u.shared = kind, False
        if kind == "qkv":
            u.parts = [(wq, fq), (wk, fk), (wv, fv)]
            u.own = lambda w: w.at[l]
            u.full = lambda f, x, c: f.at[l, x, c]
            u.half = rows_in // 2
            u.cut = lambda f, x, c, h: f.at[l, x, c, pl.ds(h * u.half, u.half)]
            u.bytes = lambda n: fg.at[0, pl.ds(0, n), 0, :, pl.ds(0, qw + 2 * kw)]
        elif kind == "o":
            u.parts = [(wo, fo)]
            u.own = lambda w: w.at[l]
            u.full = lambda f, x, c: f.at[l, x, c]
            u.half = rows_o // 2
            u.cut = lambda f, x, c, h: f.at[l, x, c, pl.ds(h * u.half, u.half)]
            u.bytes = lambda n: fo.at[0, pl.ds(0, n), 0]
        elif kind == "gu":
            col = pl.multiple_of(j * guw, guw)
            u.parts = [(wg, fg), (wu, fu)]
            u.own = lambda w: w.at[l, :, pl.ds(col, guw)]
            u.full = lambda f, x, c: f.at[l, x, c, :, pl.ds(col, guw)]
            u.half = rows_in // 2
            u.cut = lambda f, x, c, h: f.at[l, x, c, pl.ds(h * u.half, u.half), pl.ds(col, guw)]
            u.bytes = lambda n: fg.at[0, pl.ds(0, n), 0, :, pl.ds(0, 2 * guw)]
            u.shared = True
        else:
            row = pl.multiple_of(j * drows, drows)
            u.parts = [(wd, fd)]
            u.own = lambda w: w.at[l, pl.ds(row, drows)]
            u.full = lambda f, x, c: f.at[l, x, c, pl.ds(row, drows)]
            u.half = drows // 2
            u.cut = lambda f, x, c, h: f.at[l, x, c, pl.ds(pl.multiple_of(row + h * u.half, u.half), u.half)]
            u.bytes = lambda n: fd.at[0, pl.ds(0, n), 0, pl.ds(0, drows)]
            u.shared = True
        u.pair = not u.shared or not (use_z or use_y)
        u.fetch = None if u.pair else (color == j % 2)
        u.over_y = (j // 2) % 2
        return u

    def per_class(p, fn):
        l = p // per_layer
        q = p % per_layer

        @pl.when(q == 0)
        def _():
            fn(unit("qkv", l, 0), p)

        @pl.when(q == 1)
        def _():
            fn(unit("o", l, 0), p)

        @pl.when((q >= 2) & (q < 2 + gu_units))
        def _():
            fn(unit("gu", l, q - 2), p)

        @pl.when(q >= 2 + gu_units)
        def _():
            fn(unit("d", l, q - 2 - gu_units), p)

    def fetching(u, fn):
        if u.fetch is None:
            fn()
        else:
            pl.when(u.fetch)(fn)

    def on_peer(u, fn):
        if u.pair:
            return
        if use_z and use_y:
            pl.when(u.over_y == 0)(lambda: fn(z_peer))
            pl.when(u.over_y == 1)(lambda: fn(y_peer))
        else:
            fn(z_peer if use_z else y_peer)

    def wait(sem, ref):
        pltpu.make_async_copy(ref, ref, sem).wait()

    def send(src, dst, s_sem, r_sem, device):
        pltpu.make_async_remote_copy(src, dst, s_sem, r_sem, device_id=device, device_id_type=MESH).start()

    def stage_a(u, p):
        for w, f in u.parts:
            pltpu.make_async_copy(u.own(w), u.full(f, pos, core), loc.at[p]).start()

        def go():
            for w, f in u.parts:
                send(u.own(w), u.full(f, pos, core), s_own.at[p], r_left.at[p], right)
                send(u.own(w), u.full(f, pos, core), s_own.at[p], r_right.at[p], left)

        fetching(u, go)

    def stage_b(u, p):
        def go():
            wait(r_left.at[p], u.bytes(1))
            wait(r_right.at[p], u.bytes(1))
            for _, f in u.parts:
                send(u.cut(f, left_pos, core, 0), u.cut(f, left_pos, core, 0), s_rel.at[p], r_opp.at[p], right)
                send(u.cut(f, right_pos, core, 1), u.cut(f, right_pos, core, 1), s_rel.at[p], r_opp.at[p], left)

            def share(peer):
                for _, f in u.parts:
                    for x in (left_pos, right_pos):
                        send(u.full(f, x, core), u.full(f, x, core), s_par.at[p], r_par.at[p], peer)

            on_peer(u, share)

        fetching(u, go)

    def stage_c(u, p):
        def go():
            wait(r_opp.at[p], u.bytes(1))

            def share(peer):
                for _, f in u.parts:
                    send(u.full(f, opp_pos, core), u.full(f, opp_pos, core), s_par.at[p], r_par.at[p], peer)

            on_peer(u, share)

        fetching(u, go)

    def stage_n(u, p):
        if not u.pair:
            pl.when(jnp.logical_not(u.fetch))(lambda: wait(r_par.at[p], u.bytes(ring - 1)))

    def stage_d(u, p):
        wait(loc.at[p], u.bytes(1))
        for _, f in u.parts:
            src = u.full(f, pl.ds(0, ring), core)
            send(src, src, s_sib.at[p], r_sib.at[p], sibling)

    def stage_e(u, p):
        wait(r_sib.at[p], u.bytes(ring))

    def drain(u, p):
        def go():
            wait(s_own.at[p], u.bytes(2))
            wait(s_rel.at[p], u.bytes(1))
            if not u.pair:
                wait(s_par.at[p], u.bytes(ring - 1))

        fetching(u, go)
        wait(s_sib.at[p], u.bytes(ring))

    def count(v, s):
        first = jnp.clip((v + LAG[0][s]) // PACE[0], 0, per_layer)
        return first + jnp.clip((v - t_layer + LAG[1][s]) // PACE[1], 0, per_layer)

    order = [("A", stage_a), ("B", stage_b), ("C", stage_c), ("N", stage_n), ("D", stage_d)]

    att_steps, gu_steps, dn_steps = 2 * nseq, CHUNKS * nseq, nseq
    t_layer = att_steps * T_ATT + gu_steps * T_GU + dn_steps * T_DN
    steps = att_steps + gu_steps + dn_steps

    def when_of(k):
        l, i = k // steps, k % steps
        att = jnp.minimum(i, att_steps)
        gu = jnp.clip(i - att_steps, 0, gu_steps)
        dn = jnp.maximum(i - att_steps - gu_steps, 0)
        return l * t_layer + att * T_ATT + gu * T_GU + dn * T_DN

    def reached(k, s):
        l, i = k // steps, k % steps
        chunks = jnp.clip((i - att_steps + EARLY + nseq) // nseq, 1, CHUNKS)
        need = jnp.where((i >= nseq) | (l > 0), 2, 1)
        need = jnp.where(i >= att_steps - 1, 2 + SPLIT * chunks, need)
        need = jnp.where(i >= att_steps + gu_steps - 2, per_layer - LATE_D, need)
        need = jnp.where(i >= att_steps + gu_steps, per_layer + jnp.where(l + 1 < LAYERS, 1, 0), need)
        return jnp.maximum(jnp.maximum(count(when_of(k), s), l * per_layer + need), START[s])

    def tick(k):
        for s, fn in order:
            lo = jnp.where(k == 0, START[s], reached(jnp.maximum(k - 1, 0), s))
            lax.fori_loop(lo, reached(k, s), lambda p, c, fn=fn: (per_class(p, fn), c)[1], 0)

    pltpu.make_async_copy(x_in, xbuf, ld_x).start()
    first = unit("qkv", 0, 0)
    stage_a(first, 0)
    stage_b(first, 0)
    for p in range(1, START["A"]):
        q = unit("o", 0, 0) if p == 1 else unit("gu", 0, p - 2)
        stage_a(q, p)
    stage_c(first, 0)
    stage_n(first, 0)
    stage_d(first, 0)
    wait(ld_x, xbuf)

    att_o = ubuf.at[pl.ds(0, seq), pl.ds(qw + 2 * kw, qw)]
    att_h = ubuf.at[pl.ds(0, seq), pl.ds(2 * (qw + kw), dim)]

    def by_rows(fn):
        block = seq // ROW_BLOCKS
        lax.fori_loop(0, ROW_BLOCKS, lambda r, c: (fn(pl.ds(pl.multiple_of(r * block, block), block)), c)[1], 0)

    def kv_rows(s):
        return pl.ds(pl.multiple_of(s * seq, seq), seq)

    def load_gu(l, j):
        slot = j % 2
        col = pl.multiple_of(j * chunk, chunk)
        for f, b, n in ((fg, wgb, 0), (fu, wub, 1)):
            pltpu.make_async_copy(f.at[l, :, :, :, pl.ds(col, chunk)], b.at[slot], ld_gu.at[slot, n]).start()

    qkv_w = qw + 2 * kw

    def load_qkv(l):
        stage_e(unit("qkv", l, 0), l * per_layer)
        part = qkv_w // 2
        for n, (f, src, at, width) in enumerate(
            ((fq, 0, 0, part), (fq, part, part, qw - part), (fk, 0, qw, kw), (fv, 0, qw + kw, kw))
        ):
            dst = wgb.at[at // part, :, :, :, pl.ds(at % part, width)]
            pltpu.make_async_copy(f.at[l, :, :, :, pl.ds(src, width)], dst, ld_att.at[at // part]).start()

    def load_o(l):
        stage_e(unit("o", l, 0), l * per_layer + 1)
        pltpu.make_async_copy(fo.at[l], wdb.at[:, :, pl.ds(0, rows_o), :], ld_att.at[2]).start()

    def load_down(l, units):
        for n in units:
            stage_e(unit("d", l, n), l * per_layer + 2 + gu_units + n)
            at = pl.ds(n * drows, drows)
            pltpu.make_async_copy(fd.at[l, :, :, at], wdb.at[:, :, at], ld_dn).start()

    def arrive_gu(l, j):
        for n in range(SPLIT):
            stage_e(unit("gu", l, j * SPLIT + n), l * per_layer + 2 + j * SPLIT + n)

    def attention_in(l, s):
        @pl.when(s == 0)
        def _():
            @pl.when(l == 0)
            def _():
                load_qkv(0)

            for n in range(2):
                wait(ld_att.at[n], wgb.at[n])

            @pl.when(l > 0)
            def _():
                load_o(l)

        def norm(rows):
            att_h[rows, :] = rms(xbuf[s, rows, :].astype(F32), nw[l, 0:1]).astype(BF16)

        by_rows(norm)
        cos_t, sin_t = cos[l], sin[l]

        def turn(v, gain):
            v = rms(v, gain)
            lo, hi = v[:, : head // 2], v[:, head // 2 :]
            return jnp.concatenate([lo * cos_t - hi * sin_t, hi * cos_t + lo * sin_t], axis=-1).astype(BF16)

        def project(col):
            slot, col = divmod(col, qkv_w // 2)
            return dot(att_h[...], wgb[slot, :, :, :, col : col + kw].reshape(dim, kw))

        ubuf[kv_rows(s), qw : qw + kw] = turn(project(qw), qkn[l, 1:2])
        ubuf[kv_rows(s), qw + kw : qw + 2 * kw] = project(qw + kw).astype(BF16)
        for n in range(heads):
            ubuf[kv_rows(s), n * head : (n + 1) * head] = turn(project(n * head), qkn[l, 0:1])

        @pl.when(l == LAYERS - 1)
        def _():
            for f, at, n in ((k_out, qw, 0), (v_out, qw + kw, 1)):
                pltpu.make_async_copy(ubuf.at[kv_rows(s), pl.ds(at, kw)], f.at[s], st_kv.at[n, s]).start()

    def attention_out(l, s):
        @pl.when(s == 0)
        def _():
            @pl.when(l == 0)
            def _():
                load_o(0)

            wait(ld_att.at[2], fo.at[l])

        @pl.when(s == nseq - 1)
        def _():
            arrive_gu(l, 0)
            load_gu(l, 0)

        scale = head**-0.5
        blk = seq // 2
        for n in range(heads):
            for b in range(2):
                span = (b + 1) * blk
                q = ubuf[pl.ds(pl.multiple_of(s * seq + b * blk, blk), blk), n * head : (n + 1) * head]
                k = ubuf[pl.ds(pl.multiple_of(s * seq, seq), span), qw : qw + kw]
                v = ubuf[pl.ds(pl.multiple_of(s * seq, seq), span), qw + kw : qw + 2 * kw]
                sc = lax.dot_general(q, k, (((1,), (1,)), ((), ())), preferred_element_type=F32) * scale
                qpos = lax.broadcasted_iota(jnp.int32, (blk, span), 0) + b * blk
                kpos = lax.broadcasted_iota(jnp.int32, (blk, span), 1)
                sc = jnp.where(qpos >= kpos, sc, -1e30)
                e = jnp.exp(sc - jnp.max(sc, axis=-1, keepdims=True))
                pr = (e / jnp.sum(e, axis=-1, keepdims=True)).astype(BF16)
                att_o[b * blk : (b + 1) * blk, n * head : (n + 1) * head] = dot(pr, v).astype(BF16)
        for n in range(0, dim, 256):
            cols = slice(n, min(n + 256, dim))
            fbuf[:, cols] = dot(att_o[...], wdb[:, :, 0:rows_o, cols].reshape(qw, -1))

        def close(rows):
            x1 = (xbuf[s, rows, :].astype(F32) + rms(fbuf[rows, :], nw[l, 1:2])).astype(BF16)
            xbuf[s, rows, :] = x1
            gbuf[s, rows, :] = rms(x1.astype(F32), nw[l, 2:3]).astype(BF16)

        by_rows(close)

        @pl.when((s == nseq - 1) & (l == LAYERS - 1))
        def _():
            for f, at, n in ((k_out, qw, 0), (v_out, qw + kw, 1)):
                for t in range(nseq):
                    pltpu.make_async_copy(ubuf.at[kv_rows(t), pl.ds(at, kw)], f.at[t], st_kv.at[n, t]).wait()

    def gate_up(l, j, m):
        slot = j % 2

        @pl.when(m == 0)
        def _():
            for b, n in ((wgb, 0), (wub, 1)):
                wait(ld_gu.at[slot, n], b.at[slot])

        @pl.when((m == nseq - EARLY) & (j + 1 < CHUNKS))
        def _():
            arrive_gu(l, j + 1)
            load_gu(l, j + 1)

        @pl.when((j == CHUNKS - 1) & (m == nseq - 2))
        def _():
            load_down(l, range(DUNITS - LATE_D))


        step = min(256, chunk)
        for n in range(0, chunk, step):
            gate = dot(gbuf[m], wgb[slot, :, :, :, n : n + step].reshape(dim, step))
            up = dot(gbuf[m], wub[slot, :, :, :, n : n + step].reshape(dim, step))
            half = 0.5 * gate
            t = jnp.tanh(gate * (GELU_A + GELU_B * (gate * gate)))
            cols = pl.ds(pl.multiple_of(j * chunk + n, step), step)
            ubuf[kv_rows(m), cols] = ((half + half * t) * up).astype(BF16)

    def down(l, m):
        @pl.when(m == 0)
        def _():
            load_down(l, range(DUNITS - LATE_D, DUNITS))

            @pl.when(l + 1 < LAYERS)
            def _():
                load_qkv(l + 1)

            wait(ld_dn, wdb)

        for n in range(0, dim, 256):
            cols = slice(n, min(n + 256, dim))
            fbuf[:, cols] = dot(ubuf[kv_rows(m), :], wdb[:, :, :, cols].reshape(ffn, -1))

        def close(rows):
            xbuf[m, rows, :] = (xbuf[m, rows, :].astype(F32) + rms(fbuf[rows, :], nw[l, 3:4])).astype(BF16)

        by_rows(close)

        @pl.when(l == LAYERS - 1)
        def _():
            pltpu.make_async_copy(xbuf.at[m], x_out.at[m], st_x.at[m]).start()

    def body(k, carry):
        tick(k)
        l, i = k // steps, k % steps

        @pl.when(i < nseq)
        def _():
            attention_in(l, i)

        @pl.when((i >= nseq) & (i < att_steps))
        def _():
            attention_out(l, i - nseq)

        @pl.when((i >= att_steps) & (i < att_steps + gu_steps))
        def _():
            gate_up(l, (i - att_steps) // nseq, (i - att_steps) % nseq)

        @pl.when(i >= att_steps + gu_steps)
        def _():
            down(l, i - att_steps - gu_steps)

        return carry

    lax.fori_loop(0, LAYERS * steps, body, 0)

    for m in range(nseq):
        pltpu.make_async_copy(xbuf.at[m], x_out.at[m], st_x.at[m]).wait()
    lax.fori_loop(0, total, lambda p, c: (per_class(p, drain), c)[1], 0)


def layout(mesh):
    n = mesh.shape["dp"]
    lead = [getattr(d, "coords", None) for d in mesh.devices.reshape(n, -1)[:, 0]]
    nz = n
    if all(c is not None for c in lead):
        nz = next((i for i in range(1, n) if lead[i][1] != lead[0][1]), n)
    return nz, nz % 2 == 0, n % nz == 0 and (n // nz) % 2 == 0


def solution(mesh):
    batch_spec = P(("dp", "fsdp"), None, None)
    cache_spec = P(("dp", "fsdp"), None, None, None)
    weight_spec = P(None, "fsdp", None)
    rep_spec = P()
    ring = mesh.shape["fsdp"] // 2
    cfg = (ring,) + layout(mesh)

    def per_device(x, w_q, w_k, w_v, w_o, w_gate, w_up, w_down, norm_w, qk_norm_w):
        weights = (w_q, w_k, w_v, w_o, w_gate, w_up, w_down)
        nseq, seq, dim = x.shape
        head = qk_norm_w.shape[-1]
        ffn = w_gate.shape[2]
        kw = w_k.shape[2]
        assert seq <= WINDOW and kw == head and ring == 4
        cos, sin = rope_tables(seq, head)
        units = LAYERS * (2 + CHUNKS * SPLIT + DUNITS)
        hbm = pl.BlockSpec(memory_space=pl.ANY)
        vmem = pl.BlockSpec(memory_space=pltpu.VMEM)
        outs = [
            jax.ShapeDtypeStruct(x.shape, BF16),
            jax.ShapeDtypeStruct((nseq, seq, kw), BF16),
            jax.ShapeDtypeStruct((nseq, seq, kw), BF16),
        ] + [jax.ShapeDtypeStruct((LAYERS, ring, 2) + w.shape[1:], BF16) for w in weights]
        rows_d = w_down.shape[1]
        res = pl.pallas_call(
            functools.partial(kernel, cfg),
            out_shape=outs,
            in_specs=[hbm] * 8 + [vmem] * 4,
            out_specs=[hbm] * len(outs),
            scratch_shapes=[
                pltpu.VMEM((nseq, seq, dim), BF16),
                pltpu.VMEM((nseq, seq, dim), BF16),
                pltpu.VMEM((nseq * seq, ffn), BF16),
                pltpu.VMEM((seq, dim), F32),
                pltpu.VMEM((2, ring, 2, w_gate.shape[1], ffn // CHUNKS), BF16),
                pltpu.VMEM((2, ring, 2, w_gate.shape[1], ffn // CHUNKS), BF16),
                pltpu.VMEM((ring, 2, rows_d, dim), BF16),
            ]
            + [pltpu.SemaphoreType.DMA((units,)) for _ in range(10)]
            + [
                pltpu.SemaphoreType.DMA,
                pltpu.SemaphoreType.DMA((4,)),
                pltpu.SemaphoreType.DMA((2, 2)),
                pltpu.SemaphoreType.DMA,
                pltpu.SemaphoreType.DMA((2, nseq)),
                pltpu.SemaphoreType.DMA((nseq,)),
            ],
            compiler_params=pltpu.CompilerParams(
                collective_id=0, has_side_effects=True, vmem_limit_bytes=67_043_328
            ),
        )(x, *weights, norm_w, qk_norm_w, cos, sin)
        shape = (nseq, seq, 1, kw)
        return res[0], res[1].reshape(shape), res[2].reshape(shape)

    in_specs = (batch_spec,) + (weight_spec,) * 7 + (rep_spec, rep_spec)
    return jax.shard_map(per_device, mesh=mesh, in_specs=in_specs, out_specs=(batch_spec, cache_spec, cache_spec), check_vma=False)
```

```python
import functools
import math

import jax
import jax.numpy as jnp
from jax import lax
from jax.experimental import pallas as pl
from jax.experimental.pallas import tpu as pltpu
from jax.sharding import PartitionSpec as P

WINDOW = 1024
NORM_EPS = 1e-6
LOCAL_BASE = 10000.0
GLOBAL_BASE = 1000000.0
GLOBAL_POS_DIV = 8.0
MESH = pl.DeviceIdType.MESH
F32 = jnp.float32
BF16 = jnp.bfloat16
LAYERS = 2
CHUNKS = 9
SPLIT = 2
EARLY = 2
LATE_D = 2
ROW_BLOCKS = 4
DUNITS = 9
GELU_A = math.sqrt(2.0 / math.pi)
GELU_B = GELU_A * 0.044715

T_ATT, T_GU, T_DN = 34, 21, 93
PACE = (33, 32)
LAG = (dict(A=230, B=157, C=62, N=-33, D=-33), dict(A=603, B=500, C=283, N=30, D=30))
START = dict(A=4, B=1, C=1, N=1, D=1)


def rope_tables(seq_len, head_dim):
    half_dim = head_dim // 2
    exponent = -2.0 * jnp.arange(half_dim, dtype=F32) / head_dim
    inv_freq = jnp.stack([LOCAL_BASE**exponent, GLOBAL_BASE**exponent])
    positions = jnp.arange(seq_len, dtype=F32)
    positions = jnp.stack([positions, positions / GLOBAL_POS_DIV])
    angles = positions[:, :, None] * inv_freq[:, None, :]
    return jnp.cos(angles), jnp.sin(angles)


def rms(values, gain_w):
    mean_sq = jnp.mean(values * values, axis=-1, keepdims=True)
    return values * lax.rsqrt(mean_sq + NORM_EPS) * (1.0 + gain_w)


def dot(a, b):
    return jnp.dot(a, b, preferred_element_type=F32)


def kernel(cfg, x_in, wq, wk, wv, wo, wg, wu, wd, nw, qkn, cos, sin,
           x_out, k_out, v_out, fq, fk, fv, fo, fg, fu, fd,
           xbuf, gbuf, ubuf, fbuf, wgb, wub, wdb,
           loc, s_own, s_rel, s_par, s_sib, r_left, r_right, r_opp, r_par, r_sib,
           ld_x, ld_att, ld_gu, ld_dn, st_kv, st_x):
    ring, nz, use_z, use_y = cfg
    nseq, seq, dim = xbuf.shape
    rows_in, rows_o, rows_d = wq.shape[1], wo.shape[1], wd.shape[1]
    qw, kw, ffn = wq.shape[2], wk.shape[2], wg.shape[2]
    head = qkn.shape[-1]
    heads = qw // head
    chunk = ffn // CHUNKS
    gu_units = CHUNKS * SPLIT
    guw = ffn // gu_units
    drows = rows_d // DUNITS
    per_layer = 2 + gu_units + DUNITS
    total = LAYERS * per_layer

    dp = lax.axis_index("dp")
    me = lax.axis_index("fsdp")
    pos, core = me // 2, me % 2
    left_pos, right_pos = (pos + ring - 1) % ring, (pos + 1) % ring
    opp_pos = (pos + 2) % ring
    right = (dp, right_pos * 2 + core)
    left = (dp, left_pos * 2 + core)
    sibling = (dp, pos * 2 + 1 - core)
    zb = dp % 2
    yb = (dp // nz) % 2
    color = ((zb if use_z else 0) + (yb if use_y else 0)) % 2
    z_peer = (dp + 1 - 2 * zb, me)
    y_peer = (dp + nz * (1 - 2 * yb), me)
    peers = [right, left, sibling]
    if use_z:
        peers.append(z_peer)
    if use_y:
        peers.append(y_peer)

    barrier = pltpu.get_barrier_semaphore()
    for peer in peers:
        pl.semaphore_signal(barrier, inc=1, device_id=peer, device_id_type=MESH)
    pl.semaphore_wait(barrier, len(peers))

    class Unit:
        pass

    def unit(kind, l, j):
        u = Unit()
        u.kind, u.shared = kind, False
        if kind == "qkv":
            u.parts = [(wq, fq), (wk, fk), (wv, fv)]
            u.own = lambda w: w.at[l]
            u.full = lambda f, x, c: f.at[l, x, c]
            u.half = rows_in // 2
            u.cut = lambda f, x, c, h: f.at[l, x, c, pl.ds(h * u.half, u.half)]
            u.bytes = lambda n: fg.at[0, pl.ds(0, n), 0, :, pl.ds(0, qw + 2 * kw)]
        elif kind == "o":
            u.parts = [(wo, fo)]
            u.own = lambda w: w.at[l]
            u.full = lambda f, x, c: f.at[l, x, c]
            u.half = rows_o // 2
            u.cut = lambda f, x, c, h: f.at[l, x, c, pl.ds(h * u.half, u.half)]
            u.bytes = lambda n: fo.at[0, pl.ds(0, n), 0]
        elif kind == "gu":
            col = pl.multiple_of(j * guw, guw)
            u.parts = [(wg, fg), (wu, fu)]
            u.own = lambda w: w.at[l, :, pl.ds(col, guw)]
            u.full = lambda f, x, c: f.at[l, x, c, :, pl.ds(col, guw)]
            u.half = rows_in // 2
            u.cut = lambda f, x, c, h: f.at[l, x, c, pl.ds(h * u.half, u.half), pl.ds(col, guw)]
            u.bytes = lambda n: fg.at[0, pl.ds(0, n), 0, :, pl.ds(0, 2 * guw)]
            u.shared = True
        else:
            row = pl.multiple_of(j * drows, drows)
            u.parts = [(wd, fd)]
            u.own = lambda w: w.at[l, pl.ds(row, drows)]
            u.full = lambda f, x, c: f.at[l, x, c, pl.ds(row, drows)]
            u.half = drows // 2
            u.cut = lambda f, x, c, h: f.at[l, x, c, pl.ds(pl.multiple_of(row + h * u.half, u.half), u.half)]
            u.bytes = lambda n: fd.at[0, pl.ds(0, n), 0, pl.ds(0, drows)]
            u.shared = True
        u.pair = not u.shared or not (use_z or use_y)
        u.fetch = None if u.pair else (color == j % 2)
        u.over_y = (j // 2) % 2
        return u

    def per_class(p, fn):
        l = p // per_layer
        q = p % per_layer

        @pl.when(q == 0)
        def _():
            fn(unit("qkv", l, 0), p)

        @pl.when(q == 1)
        def _():
            fn(unit("o", l, 0), p)

        @pl.when((q >= 2) & (q < 2 + gu_units))
        def _():
            fn(unit("gu", l, q - 2), p)

        @pl.when(q >= 2 + gu_units)
        def _():
            fn(unit("d", l, q - 2 - gu_units), p)

    def fetching(u, fn):
        if u.fetch is None:
            fn()
        else:
            pl.when(u.fetch)(fn)

    def on_peer(u, fn):
        if u.pair:
            return
        if use_z and use_y:
            pl.when(u.over_y == 0)(lambda: fn(z_peer))
            pl.when(u.over_y == 1)(lambda: fn(y_peer))
        else:
            fn(z_peer if use_z else y_peer)

    def wait(sem, ref):
        pltpu.make_async_copy(ref, ref, sem).wait()

    def send(src, dst, s_sem, r_sem, device):
        pltpu.make_async_remote_copy(src, dst, s_sem, r_sem, device_id=device, device_id_type=MESH).start()

    def stage_a(u, p):
        for w, f in u.parts:
            pltpu.make_async_copy(u.own(w), u.full(f, pos, core), loc.at[p]).start()

        def go():
            for w, f in u.parts:
                send(u.own(w), u.full(f, pos, core), s_own.at[p], r_left.at[p], right)
                send(u.own(w), u.full(f, pos, core), s_own.at[p], r_right.at[p], left)

        fetching(u, go)

    def stage_b(u, p):
        def go():
            wait(r_left.at[p], u.bytes(1))
            wait(r_right.at[p], u.bytes(1))
            for _, f in u.parts:
                send(u.cut(f, left_pos, core, 0), u.cut(f, left_pos, core, 0), s_rel.at[p], r_opp.at[p], right)
                send(u.cut(f, right_pos, core, 1), u.cut(f, right_pos, core, 1), s_rel.at[p], r_opp.at[p], left)

            def share(peer):
                for _, f in u.parts:
                    for x in (left_pos, right_pos):
                        send(u.full(f, x, core), u.full(f, x, core), s_par.at[p], r_par.at[p], peer)

            on_peer(u, share)

        fetching(u, go)

    def stage_c(u, p):
        def go():
            wait(r_opp.at[p], u.bytes(1))

            def share(peer):
                for _, f in u.parts:
                    send(u.full(f, opp_pos, core), u.full(f, opp_pos, core), s_par.at[p], r_par.at[p], peer)

            on_peer(u, share)

        fetching(u, go)

    def stage_n(u, p):
        if not u.pair:
            pl.when(jnp.logical_not(u.fetch))(lambda: wait(r_par.at[p], u.bytes(ring - 1)))

    def stage_d(u, p):
        wait(loc.at[p], u.bytes(1))
        for _, f in u.parts:
            src = u.full(f, pl.ds(0, ring), core)
            send(src, src, s_sib.at[p], r_sib.at[p], sibling)

    def stage_e(u, p):
        wait(r_sib.at[p], u.bytes(ring))

    def drain(u, p):
        def go():
            wait(s_own.at[p], u.bytes(2))
            wait(s_rel.at[p], u.bytes(1))
            if not u.pair:
                wait(s_par.at[p], u.bytes(ring - 1))

        fetching(u, go)
        wait(s_sib.at[p], u.bytes(ring))

    def count(v, s):
        first = jnp.clip((v + LAG[0][s]) // PACE[0], 0, per_layer)
        return first + jnp.clip((v - t_layer + LAG[1][s]) // PACE[1], 0, per_layer)

    order = [("A", stage_a), ("B", stage_b), ("C", stage_c), ("N", stage_n), ("D", stage_d)]

    att_steps, gu_steps, dn_steps = 2 * nseq, CHUNKS * nseq, nseq
    t_layer = att_steps * T_ATT + gu_steps * T_GU + dn_steps * T_DN
    steps = att_steps + gu_steps + dn_steps

    def when_of(k):
        l, i = k // steps, k % steps
        att = jnp.minimum(i, att_steps)
        gu = jnp.clip(i - att_steps, 0, gu_steps)
        dn = jnp.maximum(i - att_steps - gu_steps, 0)
        return l * t_layer + att * T_ATT + gu * T_GU + dn * T_DN

    def reached(k, s):
        l, i = k // steps, k % steps
        chunks = jnp.clip((i - att_steps + EARLY + nseq) // nseq, 1, CHUNKS)
        need = jnp.where((i >= nseq) | (l > 0), 2, 1)
        need = jnp.where(i >= att_steps - 1, 2 + SPLIT * chunks, need)
        need = jnp.where(i >= att_steps + gu_steps - 2, per_layer - LATE_D, need)
        need = jnp.where(i >= att_steps + gu_steps, per_layer + jnp.where(l + 1 < LAYERS, 1, 0), need)
        return jnp.maximum(jnp.maximum(count(when_of(k), s), l * per_layer + need), START[s])

    def tick(k):
        for s, fn in order:
            lo = jnp.where(k == 0, START[s], reached(jnp.maximum(k - 1, 0), s))
            lax.fori_loop(lo, reached(k, s), lambda p, c, fn=fn: (per_class(p, fn), c)[1], 0)

    pltpu.make_async_copy(x_in, xbuf, ld_x).start()
    first = unit("qkv", 0, 0)

    def to_sibling(x):
        for _, f in first.parts:
            send(first.full(f, x, core), first.full(f, x, core), s_sib.at[0], r_sib.at[0], sibling)

    stage_a(first, 0)
    for w, f in first.parts:
        send(first.own(w), first.full(f, pos, core), s_sib.at[0], r_sib.at[0], sibling)
    stage_b(first, 0)
    to_sibling(left_pos)
    to_sibling(right_pos)
    for p in range(1, START["A"]):
        q = unit("o", 0, 0) if p == 1 else unit("gu", 0, p - 2)
        stage_a(q, p)
    stage_c(first, 0)
    to_sibling(opp_pos)
    wait(loc.at[0], first.bytes(1))
    wait(ld_x, xbuf)

    def by_rows(fn):
        block = seq // ROW_BLOCKS
        lax.fori_loop(0, ROW_BLOCKS, lambda r, c: (fn(pl.ds(pl.multiple_of(r * block, block), block)), c)[1], 0)

    def kv_rows(s):
        return pl.ds(pl.multiple_of(s * seq, seq), seq)

    def load_gu(l, j):
        slot = j % 2
        col = pl.multiple_of(j * chunk, chunk)
        for f, b, n in ((fg, wgb, 0), (fu, wub, 1)):
            pltpu.make_async_copy(f.at[l, :, :, :, pl.ds(col, chunk)], b.at[slot], ld_gu.at[slot, n]).start()

    qkv_w = qw + 2 * kw

    def load_qkv(l):
        stage_e(unit("qkv", l, 0), l * per_layer)
        part = qkv_w // 2
        for n, (f, src, at, width) in enumerate(
            ((fq, 0, 0, part), (fq, part, part, qw - part), (fk, 0, qw, kw), (fv, 0, qw + kw, kw))
        ):
            dst = wgb.at[at // part, :, :, :, pl.ds(at % part, width)]
            pltpu.make_async_copy(f.at[l, :, :, :, pl.ds(src, width)], dst, ld_att.at[at // part]).start()

    def load_o(l):
        stage_e(unit("o", l, 0), l * per_layer + 1)
        pltpu.make_async_copy(fo.at[l], wdb.at[:, :, pl.ds(0, rows_o), :], ld_att.at[2]).start()

    def load_down(l, units):
        for n in units:
            stage_e(unit("d", l, n), l * per_layer + 2 + gu_units + n)
            at = pl.ds(n * drows, drows)
            pltpu.make_async_copy(fd.at[l, :, :, at], wdb.at[:, :, at], ld_dn).start()

    def arrive_gu(l, j):
        for n in range(SPLIT):
            stage_e(unit("gu", l, j * SPLIT + n), l * per_layer + 2 + j * SPLIT + n)

    def attention_in(l, s):
        @pl.when(s == 0)
        def _():
            @pl.when(l == 0)
            def _():
                load_qkv(0)

            for n in range(2):
                wait(ld_att.at[n], wgb.at[n])

            @pl.when(l > 0)
            def _():
                load_o(l)

        def norm(rows):
            gbuf[s, rows, :] = rms(xbuf[s, rows, :].astype(F32), nw[l, 0:1]).astype(BF16)

        by_rows(norm)
        cos_t, sin_t = cos[l], sin[l]

        def turn(v, gain, scale=1.0):
            mean_sq = jnp.mean(v * v, axis=-1, keepdims=True)
            v = v * lax.rsqrt(mean_sq + NORM_EPS) * ((1.0 + gain) * scale)
            lo, hi = v[:, : head // 2], v[:, head // 2 :]
            return jnp.concatenate([lo * cos_t - hi * sin_t, hi * cos_t + lo * sin_t], axis=-1).astype(BF16)

        def project(col):
            slot, col = divmod(col, qkv_w // 2)
            return dot(gbuf[s], wgb[slot, :, :, :, col : col + kw].reshape(dim, kw))

        ubuf[kv_rows(s), qw : qw + kw] = turn(project(qw), qkn[l, 1:2])
        ubuf[kv_rows(s), qw + kw : qw + 2 * kw] = project(qw + kw).astype(BF16)
        for n in range(heads):
            ubuf[kv_rows(s), n * head : (n + 1) * head] = turn(project(n * head), qkn[l, 0:1], head**-0.5)

        @pl.when(l == LAYERS - 1)
        def _():
            for f, at, n in ((k_out, qw, 0), (v_out, qw + kw, 1)):
                pltpu.make_async_copy(ubuf.at[kv_rows(s), pl.ds(at, kw)], f.at[s], st_kv.at[n, s]).start()

    def attention_out(l, s):
        @pl.when(s == 0)
        def _():
            @pl.when(l == 0)
            def _():
                load_o(0)

            wait(ld_att.at[2], fo.at[l])

        @pl.when(s == nseq - 1)
        def _():
            arrive_gu(l, 0)
            load_gu(l, 0)

        blk = seq // 2
        for n in range(heads):
            for b in range(2):
                span = (b + 1) * blk
                q = ubuf[pl.ds(pl.multiple_of(s * seq + b * blk, blk), blk), n * head : (n + 1) * head]
                k = ubuf[pl.ds(pl.multiple_of(s * seq, seq), span), qw : qw + kw]
                v = ubuf[pl.ds(pl.multiple_of(s * seq, seq), span), qw + kw : qw + 2 * kw]
                sc = lax.dot_general(q, k, (((1,), (1,)), ((), ())), preferred_element_type=F32)
                qpos = lax.broadcasted_iota(jnp.int32, (blk, span), 0) + b * blk
                kpos = lax.broadcasted_iota(jnp.int32, (blk, span), 1)
                sc = jnp.where(qpos >= kpos, sc, -1e30)
                e = jnp.exp(sc - jnp.max(sc, axis=-1, keepdims=True))
                pr = (e / jnp.sum(e, axis=-1, keepdims=True)).astype(BF16)
                gbuf[s, b * blk : (b + 1) * blk, n * head : (n + 1) * head] = dot(pr, v).astype(BF16)
        for n in range(0, dim, 256):
            cols = slice(n, min(n + 256, dim))
            fbuf[:, cols] = dot(gbuf[s, :, 0:qw], wdb[:, :, 0:rows_o, cols].reshape(qw, -1))

        def close(rows):
            x1 = (xbuf[s, rows, :].astype(F32) + rms(fbuf[rows, :], nw[l, 1:2])).astype(BF16)
            xbuf[s, rows, :] = x1
            gbuf[s, rows, :] = rms(x1.astype(F32), nw[l, 2:3]).astype(BF16)

        by_rows(close)

        @pl.when((s == nseq - 1) & (l == LAYERS - 1))
        def _():
            for f, at, n in ((k_out, qw, 0), (v_out, qw + kw, 1)):
                for t in range(nseq):
                    pltpu.make_async_copy(ubuf.at[kv_rows(t), pl.ds(at, kw)], f.at[t], st_kv.at[n, t]).wait()

    def gate_up(l, j, m):
        slot = j % 2

        @pl.when(m == 0)
        def _():
            for b, n in ((wgb, 0), (wub, 1)):
                wait(ld_gu.at[slot, n], b.at[slot])

        @pl.when((m == nseq - EARLY) & (j + 1 < CHUNKS))
        def _():
            arrive_gu(l, j + 1)
            load_gu(l, j + 1)

        @pl.when((j == CHUNKS - 1) & (m == nseq - 2))
        def _():
            load_down(l, range(DUNITS - LATE_D))


        step = min(256, chunk)
        for n in range(0, chunk, step):
            gate = dot(gbuf[m], wgb[slot, :, :, :, n : n + step].reshape(dim, step))
            up = dot(gbuf[m], wub[slot, :, :, :, n : n + step].reshape(dim, step))
            half = 0.5 * gate
            t = jnp.tanh(gate * (GELU_A + GELU_B * (gate * gate)))
            cols = pl.ds(pl.multiple_of(j * chunk + n, step), step)
            ubuf[kv_rows(m), cols] = ((half + half * t) * up).astype(BF16)

    def down(l, m):
        @pl.when(m == 0)
        def _():
            load_down(l, range(DUNITS - LATE_D, DUNITS))

            @pl.when(l + 1 < LAYERS)
            def _():
                load_qkv(l + 1)

            wait(ld_dn, wdb)

        for n in range(0, dim, 256):
            cols = slice(n, min(n + 256, dim))
            fbuf[:, cols] = dot(ubuf[kv_rows(m), :], wdb[:, :, :, cols].reshape(ffn, -1))

        def close(rows):
            xbuf[m, rows, :] = (xbuf[m, rows, :].astype(F32) + rms(fbuf[rows, :], nw[l, 3:4])).astype(BF16)

        by_rows(close)

        @pl.when(l == LAYERS - 1)
        def _():
            pltpu.make_async_copy(xbuf.at[m], x_out.at[m], st_x.at[m]).start()

    def body(k, carry):
        tick(k)
        l, i = k // steps, k % steps

        @pl.when(i < nseq)
        def _():
            attention_in(l, i)

        @pl.when((i >= nseq) & (i < att_steps))
        def _():
            attention_out(l, i - nseq)

        @pl.when((i >= att_steps) & (i < att_steps + gu_steps))
        def _():
            gate_up(l, (i - att_steps) // nseq, (i - att_steps) % nseq)

        @pl.when(i >= att_steps + gu_steps)
        def _():
            down(l, i - att_steps - gu_steps)

        return carry

    lax.fori_loop(0, LAYERS * steps, body, 0)

    for m in range(nseq):
        pltpu.make_async_copy(xbuf.at[m], x_out.at[m], st_x.at[m]).wait()
    lax.fori_loop(0, total, lambda p, c: (per_class(p, drain), c)[1], 0)


def layout(mesh):
    n = mesh.shape["dp"]
    lead = [getattr(d, "coords", None) for d in mesh.devices.reshape(n, -1)[:, 0]]
    nz = n
    if all(c is not None for c in lead):
        nz = next((i for i in range(1, n) if lead[i][1] != lead[0][1]), n)
    return nz, nz % 2 == 0, n % nz == 0 and (n // nz) % 2 == 0


def solution(mesh):
    batch_spec = P(("dp", "fsdp"), None, None)
    cache_spec = P(("dp", "fsdp"), None, None, None)
    weight_spec = P(None, "fsdp", None)
    rep_spec = P()
    ring = mesh.shape["fsdp"] // 2
    cfg = (ring,) + layout(mesh)

    def per_device(x, w_q, w_k, w_v, w_o, w_gate, w_up, w_down, norm_w, qk_norm_w):
        weights = (w_q, w_k, w_v, w_o, w_gate, w_up, w_down)
        nseq, seq, dim = x.shape
        head = qk_norm_w.shape[-1]
        ffn = w_gate.shape[2]
        kw = w_k.shape[2]
        assert seq <= WINDOW and kw == head and ring == 4
        cos, sin = rope_tables(seq, head)
        units = LAYERS * (2 + CHUNKS * SPLIT + DUNITS)
        hbm = pl.BlockSpec(memory_space=pl.ANY)
        vmem = pl.BlockSpec(memory_space=pltpu.VMEM)
        outs = [
            jax.ShapeDtypeStruct(x.shape, BF16),
            jax.ShapeDtypeStruct((nseq, seq, kw), BF16),
            jax.ShapeDtypeStruct((nseq, seq, kw), BF16),
        ] + [jax.ShapeDtypeStruct((LAYERS, ring, 2) + w.shape[1:], BF16) for w in weights]
        rows_d = w_down.shape[1]
        res = pl.pallas_call(
            functools.partial(kernel, cfg),
            out_shape=outs,
            in_specs=[hbm] * 8 + [vmem] * 4,
            out_specs=[hbm] * len(outs),
            scratch_shapes=[
                pltpu.VMEM((nseq, seq, dim), BF16),
                pltpu.VMEM((nseq, seq, dim), BF16),
                pltpu.VMEM((nseq * seq, ffn), BF16),
                pltpu.VMEM((seq, dim), F32),
                pltpu.VMEM((2, ring, 2, w_gate.shape[1], ffn // CHUNKS), BF16),
                pltpu.VMEM((2, ring, 2, w_gate.shape[1], ffn // CHUNKS), BF16),
                pltpu.VMEM((ring, 2, rows_d, dim), BF16),
            ]
            + [pltpu.SemaphoreType.DMA((units,)) for _ in range(10)]
            + [
                pltpu.SemaphoreType.DMA,
                pltpu.SemaphoreType.DMA((4,)),
                pltpu.SemaphoreType.DMA((2, 2)),
                pltpu.SemaphoreType.DMA,
                pltpu.SemaphoreType.DMA((2, nseq)),
                pltpu.SemaphoreType.DMA((nseq,)),
            ],
            compiler_params=pltpu.CompilerParams(
                collective_id=0, has_side_effects=True, vmem_limit_bytes=67_043_328
            ),
        )(x, *weights, norm_w, qk_norm_w, cos, sin)
        shape = (nseq, seq, 1, kw)
        return res[0], res[1].reshape(shape), res[2].reshape(shape)

    in_specs = (batch_spec,) + (weight_spec,) * 7 + (rep_spec, rep_spec)
    return jax.shard_map(per_device, mesh=mesh, in_specs=in_specs, out_specs=(batch_spec, cache_spec, cache_spec), check_vma=False)
```
